32 devices in a mesh: win: 4 (over y, x), dof: 8 (over z, core).
Axes of the slice: x: 2, y: 2, z: 4, core: 2. Of those that a mesh axis runs over, the one named last changes fastest.
Arguments:
- snapshots: bfloat16 [262144, 256], P('dof', 'win'), may hold values from -6 to 6
- sketch_matrix: bfloat16 [262144, 128], P('dof'), may hold values from -0.01171875 to 0.01171875
- pivots: int32 [8, 64], P('win'), may hold values from 0 to 127
Outputs:
- singular: float32 [8, 64], P('win')
- projections: float32 [8, 64, 32], P('win')
The draws below stay inside these ranges and needn't reach their ends.
All inputs are finite; a program needn't handle non-finite values.
Results may differ from the reference program's by a relative error of at most 0.0003.
Values sent between devices are 32-bit elements; how exact they have to be, the bound alone decides.
No kernel may reach another device: no remote copies, remote signals or barrier semaphores. Data moves between devices by JAX's collectives and lax.ppermute only.
A program may use at most 64 MiB of HBM per device.

```python
import math
import jax
import jax.numpy as jnp
from jax import lax

SNAPS = 32
SKETCH = 128
RANK = 64
ORTH_ITERS = 2
WINDOWS = 8
DOFS = 262144


def set_ends(drawn, key, smallest, top_value):
    longest = drawn.shape.index(max(drawn.shape))
    spots = []
    for shift in (0, 1):
        where = [jax.random.randint(jax.random.fold_in(key, axis), (), 0, length) for axis, length in enumerate(drawn.shape)]
        where[longest] = (where[longest] + shift) % drawn.shape[longest]
        spots.append(tuple(where))
    return drawn.at[spots[0]].set(smallest).at[spots[1]].set(top_value)


def block_levels(stream_key, dims, cuts, least, largest):
    def one(axis_at, shards_of):
        steps = jax.random.uniform(jax.random.fold_in(jax.random.fold_in(stream_key, 6), axis_at), (shards_of,), jnp.float32, least / len(cuts), largest / len(cuts))
        return jnp.repeat(jnp.exp(steps), dims[axis_at] // shards_of).reshape((-1,) + (1,) * (len(dims) - axis_at - 1))

    gain = one(*cuts[0])
    for cut in cuts[1:]:
        gain = gain * one(*cut)
    return gain


def centred(stream_key, dims, width, reach, cuts=(), kind=jnp.bfloat16):
    array = width * jax.random.normal(stream_key, dims, jnp.float32)
    if cuts:
        array = array * block_levels(stream_key, dims, cuts, -0.22, 0.18)
    return jnp.clip(array, -reach, reach).astype(kind)


def setup_inputs(seed: int = 0) -> dict:
    key_of = jax.random.split(jax.random.key(seed), 4)
    snapshots = centred(key_of[0], (DOFS, WINDOWS * SNAPS), 1.0, 6.0, ((0, 8), (1, 4)))
    sketch_matrix = centred(key_of[1], (DOFS, SKETCH), DOFS ** -0.5, 0.01171875, ((0, 8),))
    pivots = set_ends(jax.random.randint(key_of[2], (WINDOWS, RANK), 0, SKETCH), jax.random.fold_in(key_of[2], 1), 0, SKETCH - 1).astype(jnp.int32)
    return {"snapshots": snapshots, "sketch_matrix": sketch_matrix, "pivots": pivots}


HIGHEST_PREC = lax.Precision.HIGHEST

def orthogonal(prefix_grams):
    batch_count = prefix_grams.shape[0]
    sketch_width = prefix_grams.shape[1]
    basis_cols = jnp.broadcast_to(jnp.eye(sketch_width, RANK, dtype=jnp.float32), (batch_count, sketch_width, RANK))
    for sweep_index in range(ORTH_ITERS):
        images = jnp.einsum('wij,wjk->wik', prefix_grams, basis_cols, precision=HIGHEST_PREC)
        inner_gram = jnp.einsum('wik,wil->wkl', images, images, precision=HIGHEST_PREC)
        chol_factor = jnp.linalg.cholesky(inner_gram)
        solved = jax.scipy.linalg.solve_triangular(chol_factor, jnp.swapaxes(images, 1, 2), lower=True)
        basis_cols = jnp.swapaxes(solved, 1, 2)
    return basis_cols

def finish(prefix_grams, basis_cols, window_blocks, pivots):
    images = jnp.einsum('wij,wjk->wik', prefix_grams, basis_cols, precision=HIGHEST_PREC)
    singular = jnp.sqrt(lax.optimization_barrier(jnp.sum(basis_cols * images, axis=1)))
    sketch_width = basis_cols.shape[1]
    pivot_table = (pivots[:, :, None] == jnp.arange(sketch_width, dtype=jnp.int32)[None, None, :]).astype(jnp.float32)
    pivot_weight = jnp.einsum('wrk,wkr->wr', pivot_table, basis_cols, precision=HIGHEST_PREC) * math.sqrt(sketch_width)
    projections = jnp.einsum('wkr,wks->wrs', basis_cols, window_blocks, precision=HIGHEST_PREC) * pivot_weight[:, :, None]
    return (singular, projections)

def reference(snapshots, sketch_matrix, pivots):
    coefficients = jnp.dot(sketch_matrix.T.astype(jnp.float32), snapshots.astype(jnp.float32), preferred_element_type=jnp.float32)
    window_blocks = jnp.transpose(coefficients.reshape(SKETCH, WINDOWS, SNAPS), (1, 0, 2))
    window_grams = jnp.einsum('wks,wjs->wkj', window_blocks, window_blocks, precision=HIGHEST_PREC)
    own_prefix = jnp.cumsum(window_grams, axis=0)
    snap_totals = (SNAPS * (jnp.arange(WINDOWS, dtype=jnp.int32) + 1)).astype(jnp.float32)
    identity = jnp.eye(SKETCH, dtype=jnp.float32)
    prefix_grams = identity[None] + own_prefix / snap_totals[:, None, None]
    basis_cols = orthogonal(prefix_grams)
    singular, projections = finish(prefix_grams, basis_cols, window_blocks, pivots)
    return (singular, projections)
```

```python
import math

import jax
import jax.numpy as jnp
from jax import lax
from jax.experimental import pallas as pl
from jax.experimental.pallas import tpu as pltpu
from jax.sharding import PartitionSpec as P


HI = lax.Precision.HIGHEST
RANK = 64
T = 8
ROLL = lambda v, s: pltpu.roll(v, s, 1)
def dot_nt(a, b, prec=HI):
    return lax.dot_general(a, b, (((1,), (1,)), ((), ())), precision=prec, preferred_element_type=jnp.float32)
def dot_nn(a, b, prec=HI):
    return lax.dot_general(a, b, (((1,), (0,)), ((), ())), precision=prec, preferred_element_type=jnp.float32)
def sb(v, k):
    return jnp.broadcast_to(v[k:k+1, :], v.shape)
GATHER = True
def col(v, k, low, half):
    if GATHER:
        idx = jnp.where(low, k, k + half)
        return jnp.take_along_axis(v, idx, axis=1, mode="promise_in_bounds")
    return jnp.where(low, jnp.broadcast_to(v[:, k:k+1], v.shape), jnp.broadcast_to(v[:, k+half:k+half+1], v.shape))
LOOK = True
def eliminate(gram, sides):
    n = len(gram)
    width = gram[0].shape[1]; half = width // 2
    lane = lax.broadcasted_iota(jnp.int32, gram[0].shape, 1)
    sub = lax.broadcasted_iota(jnp.int32, gram[0].shape, 0)
    low = lane < half
    gram = list(gram); sides = [list(s) for s in sides]
    ahead = None
    for p in range(n):
        cols = {}
        for r in range(p, n):
            if r == p and ahead is not None: cols[r] = ahead
            else: cols[r] = [col(gram[r], T*p + j, low, half) for j in range(T)]
        nxt = None
        if LOOK and p + 1 < n: nxt = [col(gram[p+1], T*(p+1) + j, low, half) for j in range(T)]
        pivots = None
        arrs = sides + ([gram] if p + 1 < n else [])
        for k in range(T):
            piv = sb(cols[p][k], k)
            inv = 1.0 / piv
            pivots = piv if k == 0 else jnp.where(sub == k, piv, pivots)
            mult = {}
            for r in range(p, n):
                m = cols[r][k] * inv
                mult[r] = jnp.where(sub > k, m, 0.0) if r == p else m
            for j in range(k+1, T):
                e = sb(cols[p][j], k)
                for r in range(p, n):
                    cols[r][j] = cols[r][j] - mult[r] * e
            if nxt is not None:
                for j in range(T):
                    nxt[j] = nxt[j] - mult[p+1] * sb(cols[p+1][k], j)
            for a in arrs:
                row = sb(a[p], k)
                for r in range(p, n):
                    a[r] = a[r] - mult[r] * row
        scale = lax.rsqrt(pivots)
        for s in sides: s[p] = s[p] * scale
        ahead = nxt
    return sides
def tiles(a): return [a[T*i:T*(i+1)] for i in range(a.shape[0]//T)]
def side_by_side(a, b, low, half):
    return jnp.where(low, a, ROLL(b, half)), jnp.where(low, ROLL(a, half), b)
def orth(x0, x1, low, half):
    both = jnp.concatenate([x0, x1], axis=0)
    g = dot_nt(both, both)
    n = x0.shape[0]
    gram = jnp.where(low, g[:n], g[n:])
    lo, hi = side_by_side(x0, x1, low, half)
    lo, hi = eliminate(tiles(gram), [tiles(lo), tiles(hi)])
    lo = jnp.concatenate(lo, axis=0); hi = jnp.concatenate(hi, axis=0)
    return side_by_side(lo, hi, low, half)
def la_core(win, blocks, piv, nwin_here):
    width = blocks[0].shape[1]; half = width // 2
    cols_here = blocks[0].shape[0]; snaps = cols_here // nwin_here
    full = jnp.concatenate(blocks, axis=0)
    total = full.shape[0]
    rowid = lax.broadcasted_iota(jnp.int32, (1, total), 1)
    rel = rowid // cols_here
    earlier = jnp.logical_and(rel > 0, (jnp.bitwise_xor(rel, win)) < win)
    keep = [jnp.logical_or(earlier, rowid < snaps * (w + 1)) for w in range(nwin_here)]
    ft = full.T
    lhs = jnp.concatenate([jnp.where(k, ft, 0.0) for k in keep], axis=0)
    sums = dot_nn(lhs, full)
    eye = (lax.broadcasted_iota(jnp.int32, (width, width), 0) == lax.broadcasted_iota(jnp.int32, (width, width), 1)).astype(jnp.float32)
    grams = []
    for w in range(nwin_here):
        c = (snaps * (win * nwin_here + w + 1)).astype(jnp.float32)
        grams.append(eye + sums[width*w:width*(w+1)] / c)
    low = lax.broadcasted_iota(jnp.int32, (RANK, width), 1) < half
    b0, b1 = orth(grams[0][:RANK], grams[1][:RANK], low, half)
    b0, b1 = orth(dot_nn(b0, grams[0]), dot_nn(b1, grams[1]), low, half)
    ones = jnp.ones((T, width), jnp.float32)
    lane = lax.broadcasted_iota(jnp.int32, (RANK, width), 1).astype(jnp.float32)
    sing, proj = [], []
    for w, b in enumerate((b0, b1)):
        img = dot_nn(b, grams[w])
        s = dot_nt(ones, b * img)[:1]
        sing.append(jnp.sqrt(s))
        pv = jnp.broadcast_to(piv[w:w+1, :].astype(jnp.float32), (width, RANK)).T
        pw = dot_nt(ones, jnp.where(lane == pv, b, 0.0))[:1] * math.sqrt(width)
        pr = dot_nt(blocks[0][snaps*w:snaps*(w+1)], b)
        proj.append(pr * jnp.broadcast_to(pw, pr.shape))
    return sing, proj


CHUNKS = 16


def sketch_kernel(snap_ref, sketch_ref, out_ref, snap_buf, sketch_buf, sems):
    step = sketch_buf.shape[0] // CHUNKS
    copies = []
    for i in range(CHUNKS):
        rows = pl.ds(i * step, step)
        pair = (
            pltpu.make_async_copy(snap_ref.at[:, rows], snap_buf.at[:, rows], sems.at[0, i]),
            pltpu.make_async_copy(sketch_ref.at[rows, :], sketch_buf.at[rows, :], sems.at[1, i]),
        )
        for copy in pair:
            copy.start()
        copies.append(pair)
    total = None
    for i in range(CHUNKS):
        for copy in copies[i]:
            copy.wait()
        rows = pl.ds(i * step, step)
        part = jnp.dot(snap_buf[:, rows], sketch_buf[rows, :], preferred_element_type=jnp.float32)
        total = part if i == 0 else total + part
    out_ref[...] = total


def sketch_product(snapshots, sketch_matrix):
    dofs, cols = snapshots.shape
    width = sketch_matrix.shape[1]
    return pl.pallas_call(
        sketch_kernel,
        in_specs=[pl.BlockSpec(memory_space=pl.ANY)] * 2,
        out_specs=pl.BlockSpec(memory_space=pltpu.VMEM),
        out_shape=jax.ShapeDtypeStruct((cols, width), jnp.float32),
        scratch_shapes=[
            pltpu.VMEM((cols, dofs), snapshots.dtype),
            pltpu.VMEM((dofs, width), sketch_matrix.dtype),
            pltpu.SemaphoreType.DMA((2, CHUNKS)),
        ],
        name="sketch_product",
    )(snapshots.T, sketch_matrix)


def solve_kernel(windows_here, *refs):
    *block_refs, pivot_ref, singular_ref, projection_ref = refs
    sing, proj = la_core(lax.axis_index("win"), [r[...] for r in block_refs], pivot_ref[...], windows_here)
    for w in range(windows_here):
        singular_ref[w : w + 1, :] = sing[w]
        projection_ref[w] = proj[w]


def solve(blocks, pivots):
    windows_here = pivots.shape[0]
    snaps = blocks[0].shape[0] // windows_here
    singular, projections = pl.pallas_call(
        lambda *refs: solve_kernel(windows_here, *refs),
        in_specs=[pl.BlockSpec(memory_space=pltpu.VMEM)] * (len(blocks) + 1),
        out_specs=[pl.BlockSpec(memory_space=pltpu.VMEM)] * 2,
        out_shape=[
            jax.ShapeDtypeStruct((windows_here, RANK), jnp.float32),
            jax.ShapeDtypeStruct((windows_here, snaps, RANK), jnp.float32),
        ],
        name="solve_windows",
    )(*blocks, pivots)
    return singular, jnp.transpose(projections, (0, 2, 1))


def solution(mesh):
    win_count, dof_count = mesh.shape["win"], mesh.shape["dof"]

    def exchange(value, axis, step):
        count = mesh.shape[axis]
        return lax.ppermute(value, axis, [(i, i ^ step) for i in range(count)])

    def local(snapshots, sketch_matrix, pivots):
        coeffs = sketch_product(snapshots, sketch_matrix)
        step = 1
        while step < dof_count:
            coeffs = coeffs + exchange(coeffs, "dof", step)
            step *= 2
        blocks = [coeffs] + [exchange(coeffs, "win", k) for k in range(1, win_count)]
        return solve(blocks, pivots)

    return jax.shard_map(
        local,
        mesh=mesh,
        in_specs=(P("dof", "win"), P("dof", None), P("win", None)),
        out_specs=(P("win", None), P("win", None, None)),
        check_vma=False,
    )
```

```python
import math

import jax
import jax.numpy as jnp
from jax import lax
from jax.experimental import pallas as pl
from jax.experimental.pallas import tpu as pltpu
from jax.sharding import PartitionSpec as P


HI = lax.Precision.HIGHEST
RANK = 64
T = 8
ROLL = lambda v, s: pltpu.roll(v, s, 1)
def dot_nt(a, b, prec=HI):
    return lax.dot_general(a, b, (((1,), (1,)), ((), ())), precision=prec, preferred_element_type=jnp.float32)
def dot_nn(a, b, prec=HI):
    return lax.dot_general(a, b, (((1,), (0,)), ((), ())), precision=prec, preferred_element_type=jnp.float32)
def sb(v, k):
    return jnp.broadcast_to(v[k:k+1, :], v.shape)
GATHER = True
def col(v, k, low, half):
    if GATHER:
        idx = jnp.where(low, k, k + half)
        return jnp.take_along_axis(v, idx, axis=1, mode="promise_in_bounds")
    return jnp.where(low, jnp.broadcast_to(v[:, k:k+1], v.shape), jnp.broadcast_to(v[:, k+half:k+half+1], v.shape))
LOOK = True
def eliminate(gram, sides):
    n = len(gram)
    width = gram[0].shape[1]; half = width // 2
    lane = lax.broadcasted_iota(jnp.int32, gram[0].shape, 1)
    sub = lax.broadcasted_iota(jnp.int32, gram[0].shape, 0)
    low = lane < half
    gram = list(gram); sides = [list(s) for s in sides]
    ahead = None
    for p in range(n):
        cols = {}
        for r in range(p, n):
            if r == p and ahead is not None: cols[r] = ahead
            else: cols[r] = [col(gram[r], T*p + j, low, half) for j in range(T)]
        nxt = None
        if LOOK and p + 1 < n: nxt = [col(gram[p+1], T*(p+1) + j, low, half) for j in range(T)]
        pivots = None
        arrs = sides + ([gram] if p + 1 < n else [])
        for k in range(T):
            piv = sb(cols[p][k], k)
            inv = 1.0 / piv
            pivots = piv if k == 0 else jnp.where(sub == k, piv, pivots)
            mult = {}
            for r in range(p, n):
                m = cols[r][k] * inv
                mult[r] = jnp.where(sub > k, m, 0.0) if r == p else m
            for j in range(k+1, T):
                e = sb(cols[p][j], k)
                for r in range(p, n):
                    cols[r][j] = cols[r][j] - mult[r] * e
            if nxt is not None:
                for j in range(T):
                    nxt[j] = nxt[j] - mult[p+1] * sb(cols[p+1][k], j)
            for a in arrs:
                row = sb(a[p], k)
                for r in range(p, n):
                    a[r] = a[r] - mult[r] * row
        scale = lax.rsqrt(pivots)
        for s in sides: s[p] = s[p] * scale
        ahead = nxt
    return sides
def tiles(a): return [a[T*i:T*(i+1)] for i in range(a.shape[0]//T)]
def side_by_side(a, b, low, half):
    return jnp.where(low, a, ROLL(b, half)), jnp.where(low, ROLL(a, half), b)
def orth(x0, x1, low, half):
    both = jnp.concatenate([x0, x1], axis=0)
    g = dot_nt(both, both)
    n = x0.shape[0]
    gram = jnp.where(low, g[:n], g[n:])
    lo, hi = side_by_side(x0, x1, low, half)
    lo, hi = eliminate(tiles(gram), [tiles(lo), tiles(hi)])
    lo = jnp.concatenate(lo, axis=0); hi = jnp.concatenate(hi, axis=0)
    return side_by_side(lo, hi, low, half)
def la_core(win, blocks, piv, nwin_here):
    width = blocks[0].shape[1]; half = width // 2
    cols_here = blocks[0].shape[0]; snaps = cols_here // nwin_here
    full = jnp.concatenate(blocks, axis=0)
    total = full.shape[0]
    rowid = lax.broadcasted_iota(jnp.int32, (1, total), 1)
    rel = rowid // cols_here
    earlier = jnp.logical_and(rel > 0, (jnp.bitwise_xor(rel, win)) < win)
    keep = [jnp.logical_or(earlier, rowid < snaps * (w + 1)) for w in range(nwin_here)]
    ft = full.T
    lhs = jnp.concatenate([jnp.where(k, ft, 0.0) for k in keep], axis=0)
    sums = dot_nn(lhs, full)
    eye = (lax.broadcasted_iota(jnp.int32, (width, width), 0) == lax.broadcasted_iota(jnp.int32, (width, width), 1)).astype(jnp.float32)
    grams = []
    for w in range(nwin_here):
        c = (snaps * (win * nwin_here + w + 1)).astype(jnp.float32)
        grams.append(eye + sums[width*w:width*(w+1)] / c)
    low = lax.broadcasted_iota(jnp.int32, (RANK, width), 1) < half
    b0, b1 = orth(grams[0][:RANK], grams[1][:RANK], low, half)
    b0, b1 = orth(dot_nn(b0, grams[0]), dot_nn(b1, grams[1]), low, half)
    ones = jnp.ones((T, width), jnp.float32)
    lane = lax.broadcasted_iota(jnp.int32, (RANK, width), 1).astype(jnp.float32)
    sing, proj = [], []
    for w, b in enumerate((b0, b1)):
        img = dot_nn(b, grams[w])
        s = dot_nt(ones, b * img)[:1]
        sing.append(jnp.sqrt(s))
        pv = jnp.broadcast_to(piv[w:w+1, :].astype(jnp.float32), (width, RANK)).T
        pw = dot_nt(ones, jnp.where(lane == pv, b, 0.0))[:1] * math.sqrt(width)
        pr = dot_nt(blocks[0][snaps*w:snaps*(w+1)], b)
        proj.append(pr * jnp.broadcast_to(pw, pr.shape))
    return sing, proj


CHUNKS = 16


def sketch_kernel(snap_ref, sketch_ref, out_ref, snap_buf, sketch_buf, sems):
    step = sketch_buf.shape[0] // CHUNKS
    copies = []
    for i in range(CHUNKS):
        rows = pl.ds(i * step, step)
        pair = (
            pltpu.make_async_copy(snap_ref.at[:, rows], snap_buf.at[:, rows], sems.at[0, i]),
            pltpu.make_async_copy(sketch_ref.at[rows, :], sketch_buf.at[rows, :], sems.at[1, i]),
        )
        for copy in pair:
            copy.start()
        copies.append(pair)
    total = None
    for i in range(CHUNKS):
        for copy in copies[i]:
            copy.wait()
        rows = pl.ds(i * step, step)
        part = jnp.dot(snap_buf[:, rows], sketch_buf[rows, :], preferred_element_type=jnp.float32)
        total = part if i == 0 else total + part
    out_ref[...] = total


def sketch_product(snapshots, sketch_matrix):
    dofs, cols = snapshots.shape
    width = sketch_matrix.shape[1]
    return pl.pallas_call(
        sketch_kernel,
        in_specs=[pl.BlockSpec(memory_space=pltpu.HBM)] * 2,
        out_specs=pl.BlockSpec(memory_space=pltpu.VMEM),
        out_shape=jax.ShapeDtypeStruct((cols, width), jnp.float32),
        scratch_shapes=[
            pltpu.VMEM((cols, dofs), snapshots.dtype),
            pltpu.VMEM((dofs, width), sketch_matrix.dtype),
            pltpu.SemaphoreType.DMA((2, CHUNKS)),
        ],
        compiler_params=pltpu.CompilerParams(vmem_limit_bytes=52 * 2**20),
        name="sketch_product",
    )(snapshots.T, sketch_matrix)


def solve_kernel(windows_here, *refs):
    *block_refs, pivot_ref, singular_ref, projection_ref = refs
    sing, proj = la_core(lax.axis_index("win"), [r[...] for r in block_refs], pivot_ref[...], windows_here)
    for w in range(windows_here):
        singular_ref[w : w + 1, :] = sing[w]
        projection_ref[w] = proj[w]


def solve(blocks, pivots):
    windows_here = pivots.shape[0]
    snaps = blocks[0].shape[0] // windows_here
    singular, projections = pl.pallas_call(
        lambda *refs: solve_kernel(windows_here, *refs),
        in_specs=[pl.BlockSpec(memory_space=pltpu.VMEM)] * (len(blocks) + 1),
        out_specs=[pl.BlockSpec(memory_space=pltpu.VMEM)] * 2,
        out_shape=[
            jax.ShapeDtypeStruct((windows_here, RANK), jnp.float32),
            jax.ShapeDtypeStruct((windows_here, snaps, RANK), jnp.float32),
        ],
        compiler_params=pltpu.CompilerParams(vmem_limit_bytes=8 * 2**20),
        name="solve_windows",
    )(*blocks, pivots)
    return singular, jnp.transpose(projections, (0, 2, 1))


def solution(mesh):
    win_count, dof_count = mesh.shape["win"], mesh.shape["dof"]

    def exchange(value, axis, step):
        count = mesh.shape[axis]
        return lax.ppermute(value, axis, [(i, i ^ step) for i in range(count)])

    def local(snapshots, sketch_matrix, pivots):
        coeffs = sketch_product(snapshots, sketch_matrix)
        step = 1
        while step < dof_count:
            coeffs = coeffs + exchange(coeffs, "dof", step)
            step *= 2
        blocks = [coeffs] + [exchange(coeffs, "win", k) for k in range(1, win_count)]
        return solve(blocks, pivots)

    return jax.shard_map(
        local,
        mesh=mesh,
        in_specs=(P("dof", "win"), P("dof", None), P("win", None)),
        out_specs=(P("win", None), P("win", None, None)),
        check_vma=False,
    )
```

```python
import math

import jax
import jax.numpy as jnp
from jax import lax
from jax.experimental import pallas as pl
from jax.experimental.pallas import tpu as pltpu
from jax.sharding import PartitionSpec as P


HI = lax.Precision.HIGHEST
RANK = 64
T = 8
ROLL = lambda v, s: pltpu.roll(v, s, 1)
def dot_nt(a, b, prec=HI):
    return lax.dot_general(a, b, (((1,), (1,)), ((), ())), precision=prec, preferred_element_type=jnp.float32)
def dot_nn(a, b, prec=HI):
    return lax.dot_general(a, b, (((1,), (0,)), ((), ())), precision=prec, preferred_element_type=jnp.float32)
def sb(v, k):
    return jnp.broadcast_to(v[k:k+1, :], v.shape)
GATHER = True
def col(v, k, low, half):
    if GATHER:
        idx = jnp.where(low, k, k + half)
        return jnp.take_along_axis(v, idx, axis=1, mode="promise_in_bounds")
    return jnp.where(low, jnp.broadcast_to(v[:, k:k+1], v.shape), jnp.broadcast_to(v[:, k+half:k+half+1], v.shape))
LOOK = True
def eliminate(gram, sides):
    n = len(gram)
    width = gram[0].shape[1]; half = width // 2
    lane = lax.broadcasted_iota(jnp.int32, gram[0].shape, 1)
    sub = lax.broadcasted_iota(jnp.int32, gram[0].shape, 0)
    low = lane < half
    gram = list(gram); sides = [list(s) for s in sides]
    ahead = None
    for p in range(n):
        cols = {}
        for r in range(p, n):
            if r == p and ahead is not None: cols[r] = ahead
            else: cols[r] = [col(gram[r], T*p + j, low, half) for j in range(T)]
        nxt = None
        if LOOK and p + 1 < n: nxt = [col(gram[p+1], T*(p+1) + j, low, half) for j in range(T)]
        pivots = None
        arrs = sides + ([gram] if p + 1 < n else [])
        for k in range(T):
            piv = sb(cols[p][k], k)
            inv = 1.0 / piv
            pivots = piv if k == 0 else jnp.where(sub == k, piv, pivots)
            mult = {}
            for r in range(p, n):
                m = cols[r][k] * inv
                mult[r] = jnp.where(sub > k, m, 0.0) if r == p else m
            for j in range(k+1, T):
                e = sb(cols[p][j], k)
                for r in range(p, n):
                    cols[r][j] = cols[r][j] - mult[r] * e
            if nxt is not None:
                for j in range(T):
                    nxt[j] = nxt[j] - mult[p+1] * sb(cols[p+1][k], j)
            for a in arrs:
                row = sb(a[p], k)
                for r in range(p, n):
                    a[r] = a[r] - mult[r] * row
        scale = lax.rsqrt(pivots)
        for s in sides: s[p] = s[p] * scale
        ahead = nxt
    return sides
def tiles(a): return [a[T*i:T*(i+1)] for i in range(a.shape[0]//T)]
def side_by_side(a, b, low, half):
    return jnp.where(low, a, ROLL(b, half)), jnp.where(low, ROLL(a, half), b)
def orth(x0, x1, low, half):
    both = jnp.concatenate([x0, x1], axis=0)
    g = dot_nt(both, both)
    n = x0.shape[0]
    gram = jnp.where(low, g[:n], g[n:])
    lo, hi = side_by_side(x0, x1, low, half)
    lo, hi = eliminate(tiles(gram), [tiles(lo), tiles(hi)])
    lo = jnp.concatenate(lo, axis=0); hi = jnp.concatenate(hi, axis=0)
    return side_by_side(lo, hi, low, half)
def la_core(win, blocks, piv, nwin_here):
    width = blocks[0].shape[1]; half = width // 2
    cols_here = blocks[0].shape[0]; snaps = cols_here // nwin_here
    full = jnp.concatenate(blocks, axis=0)
    total = full.shape[0]
    rowid = lax.broadcasted_iota(jnp.int32, (1, total), 1)
    rel = rowid // cols_here
    earlier = jnp.logical_and(rel > 0, (jnp.bitwise_xor(rel, win)) < win)
    keep = [jnp.logical_or(earlier, rowid < snaps * (w + 1)) for w in range(nwin_here)]
    ft = full.T
    lhs = jnp.concatenate([jnp.where(k, ft, 0.0) for k in keep], axis=0)
    sums = dot_nn(lhs, full)
    eye = (lax.broadcasted_iota(jnp.int32, (width, width), 0) == lax.broadcasted_iota(jnp.int32, (width, width), 1)).astype(jnp.float32)
    grams = []
    for w in range(nwin_here):
        c = (snaps * (win * nwin_here + w + 1)).astype(jnp.float32)
        grams.append(eye + sums[width*w:width*(w+1)] / c)
    low = lax.broadcasted_iota(jnp.int32, (RANK, width), 1) < half
    b0, b1 = orth(grams[0][:RANK], grams[1][:RANK], low, half)
    b0, b1 = orth(dot_nn(b0, grams[0]), dot_nn(b1, grams[1]), low, half)
    ones = jnp.ones((T, width), jnp.float32)
    lane = lax.broadcasted_iota(jnp.int32, (RANK, width), 1).astype(jnp.float32)
    sing, proj = [], []
    for w, b in enumerate((b0, b1)):
        img = dot_nn(b, grams[w])
        s = dot_nt(ones, b * img)[:1]
        sing.append(jnp.sqrt(s))
        pv = jnp.broadcast_to(piv[w:w+1, :].astype(jnp.float32), (width, RANK)).T
        pw = dot_nt(ones, jnp.where(lane == pv, b, 0.0))[:1] * math.sqrt(width)
        pr = dot_nt(blocks[0][snaps*w:snaps*(w+1)], b)
        proj.append(pr * jnp.broadcast_to(pw, pr.shape))
    return sing, proj


CHUNKS = 16


def sketch_kernel(snap_ref, sketch_ref, out_ref, snap_buf, sketch_buf, sems):
    step = sketch_buf.shape[0] // CHUNKS
    copies = []
    for i in range(CHUNKS):
        rows = pl.ds(i * step, step)
        pair = (
            pltpu.make_async_copy(snap_ref.at[:, rows], snap_buf.at[:, rows], sems.at[0, i]),
            pltpu.make_async_copy(sketch_ref.at[rows, :], sketch_buf.at[rows, :], sems.at[1, i]),
        )
        for copy in pair:
            copy.start()
        copies.append(pair)
    total = None
    for i in range(CHUNKS):
        for copy in copies[i]:
            copy.wait()
        rows = pl.ds(i * step, step)
        part = jnp.dot(snap_buf[:, rows], sketch_buf[rows, :], preferred_element_type=jnp.float32)
        total = part if i == 0 else total + part
    out_ref[...] = total


def sketch_product(snapshots, sketch_matrix):
    dofs, cols = snapshots.shape
    width = sketch_matrix.shape[1]
    return pl.pallas_call(
        sketch_kernel,
        in_specs=[pl.BlockSpec(memory_space=pltpu.HBM)] * 2,
        out_specs=pl.BlockSpec(memory_space=pltpu.VMEM),
        out_shape=jax.ShapeDtypeStruct((cols, width), jnp.float32),
        scratch_shapes=[
            pltpu.VMEM((cols, dofs), snapshots.dtype),
            pltpu.VMEM((dofs, width), sketch_matrix.dtype),
            pltpu.SemaphoreType.DMA((2, CHUNKS)),
        ],
        compiler_params=pltpu.CompilerParams(vmem_limit_bytes=52 * 2**20),
        name="sketch_product",
    )(snapshots.T, sketch_matrix)


def solve_kernel(windows_here, *refs):
    *block_refs, pivot_ref, singular_ref, projection_ref = refs
    sing, proj = la_core(lax.axis_index("win"), [r[...] for r in block_refs], pivot_ref[...], windows_here)
    for w in range(windows_here):
        singular_ref[w : w + 1, :] = sing[w]
        projection_ref[w] = proj[w]


def solve(blocks, pivots):
    windows_here = pivots.shape[0]
    snaps = blocks[0].shape[0] // windows_here
    singular, projections = pl.pallas_call(
        lambda *refs: solve_kernel(windows_here, *refs),
        in_specs=[pl.BlockSpec(memory_space=pltpu.VMEM)] * (len(blocks) + 1),
        out_specs=[pl.BlockSpec(memory_space=pltpu.VMEM)] * 2,
        out_shape=[
            jax.ShapeDtypeStruct((windows_here, RANK), jnp.float32),
            jax.ShapeDtypeStruct((windows_here, snaps, RANK), jnp.float32),
        ],
        compiler_params=pltpu.CompilerParams(vmem_limit_bytes=8 * 2**20),
        name="solve_windows",
    )(*blocks, pivots)
    return singular, jnp.transpose(projections, (0, 2, 1))


def solution(mesh):
    win_count, dof_count = mesh.shape["win"], mesh.shape["dof"]

    def hop(value, win_step, dof_step):
        pairs = [
            (w * dof_count + d, (w ^ win_step) * dof_count + (d ^ dof_step))
            for w in range(win_count)
            for d in range(dof_count)
        ]
        return lax.ppermute(value, ("win", "dof"), pairs)

    def local(snapshots, sketch_matrix, pivots):
        coeffs = sketch_product(snapshots, sketch_matrix)
        coeffs = coeffs + hop(coeffs, 0, 1)
        step = 2
        while step < dof_count:
            coeffs = coeffs + hop(coeffs, 0, step + 1)
            step *= 2
        blocks = [coeffs] + [hop(coeffs, k, 1) for k in range(1, win_count)]
        return solve(blocks, pivots)

    return jax.shard_map(
        local,
        mesh=mesh,
        in_specs=(P("dof", "win"), P("dof", None), P("win", None)),
        out_specs=(P("win", None), P("win", None, None)),
        check_vma=False,
    )
```

```python
import math

import jax
import jax.numpy as jnp
from jax import lax
from jax.experimental import pallas as pl
from jax.experimental.pallas import tpu as pltpu
from jax.sharding import PartitionSpec as P


HI = lax.Precision.HIGHEST
RANK = 64
T = 8
ROLL = lambda v, s: pltpu.roll(v, s, 1)
def split(x):
    high = x.astype(jnp.bfloat16)
    rest = x - high.astype(jnp.float32)
    mid = rest.astype(jnp.bfloat16)
    return high, mid, (rest - mid.astype(jnp.float32)).astype(jnp.bfloat16)


def product(a, b, transposed=False):
    ah, am, al = split(a) if not isinstance(a, tuple) else a
    bh, bm, bl = split(b) if not isinstance(b, tuple) else b
    axis = 1 if transposed else 0
    left = jnp.concatenate([ah, ah, am, ah, am, al], axis=1)
    right = jnp.concatenate([bh, bm, bh, bl, bm, bh], axis=axis)
    return lax.dot_general(left, right, (((1,), (axis,)), ((), ())), preferred_element_type=jnp.float32)


def sb(v, k):
    return jnp.broadcast_to(v[k:k+1, :], v.shape)
GATHER = True
def col(v, k, low, half):
    if GATHER:
        idx = jnp.where(low, k, k + half)
        return jnp.take_along_axis(v, idx, axis=1, mode="promise_in_bounds")
    return jnp.where(low, jnp.broadcast_to(v[:, k:k+1], v.shape), jnp.broadcast_to(v[:, k+half:k+half+1], v.shape))
def eliminate(gram):
    n = len(gram)
    width = gram[0].shape[1]
    half = width // 2
    lane = lax.broadcasted_iota(jnp.int32, gram[0].shape, 1)
    sub = lax.broadcasted_iota(jnp.int32, gram[0].shape, 0)
    low = lane < half
    column = jnp.where(low, lane, lane - half)
    gram = list(gram)
    ahead = None
    for p in range(n):
        cols = {}
        for r in range(p, n):
            if r == p and ahead is not None:
                cols[r] = ahead
            else:
                cols[r] = [col(gram[r], T * p + j, low, half) for j in range(T)]
        nxt = None
        if p + 1 < n:
            nxt = [col(gram[p + 1], T * (p + 1) + j, low, half) for j in range(T)]
        done = jnp.logical_and(column >= T * p, column < T * (p + 1))
        gram[p] = jnp.where(done, jnp.where(sub == column - T * p, 1.0, 0.0), gram[p])
        for r in range(p + 1, n):
            gram[r] = jnp.where(done, 0.0, gram[r])
        pivots = None
        for k in range(T):
            piv = sb(cols[p][k], k)
            inv = 1.0 / piv
            pivots = piv if k == 0 else jnp.where(sub == k, piv, pivots)
            mult = {}
            for r in range(p, n):
                m = cols[r][k] * inv
                mult[r] = jnp.where(sub > k, m, 0.0) if r == p else m
            for j in range(k + 1, T):
                e = sb(cols[p][j], k)
                for r in range(p, n):
                    cols[r][j] = cols[r][j] - mult[r] * e
            if nxt is not None:
                for j in range(T):
                    nxt[j] = nxt[j] - mult[p + 1] * sb(cols[p + 1][k], j)
            row = sb(gram[p], k)
            for r in range(p, n):
                gram[r] = gram[r] - mult[r] * row
        gram[p] = jnp.where(column < T * (p + 1), gram[p] * lax.rsqrt(pivots), 0.0)
        ahead = nxt
    return gram


def tiles(a): return [a[T*i:T*(i+1)] for i in range(a.shape[0]//T)]
def diagonal_blocks(square, low):
    n = square.shape[0] // 2
    return jnp.where(low, square[:n], square[n:])


def block_diagonal(pair, low):
    return jnp.concatenate([jnp.where(low, pair, 0.0), jnp.where(low, 0.0, pair)], axis=0)


def inverse_factor(images, low):
    pair = diagonal_blocks(product(images, images, transposed=True), low)
    return jnp.concatenate(eliminate(tiles(pair)), axis=0)


def la_core(win, blocks, rels, piv, nwin_here):
    width = blocks[0].shape[1]
    half = width // 2
    own = blocks[0]
    snaps = own.shape[0] // 2
    others = [jnp.where(jnp.bitwise_xor(win, rel) < win, b, 0.0) for b, rel in zip(blocks[1:], rels[1:])]
    full = jnp.concatenate(blocks, axis=0)
    kept = [
        jnp.concatenate([own[:snaps], jnp.zeros((snaps, width), jnp.float32)] + others, axis=0),
        jnp.concatenate([own] + others, axis=0),
    ]
    sums = product(full.T, jnp.concatenate(kept, axis=1))
    eye = (
        lax.broadcasted_iota(jnp.int32, (width, width), 0) == lax.broadcasted_iota(jnp.int32, (width, width), 1)
    ).astype(jnp.float32)
    grams = [
        eye + sums[:, width * w : width * (w + 1)] / (snaps * (win * 2 + w + 1)).astype(jnp.float32) for w in range(2)
    ]
    low = lax.broadcasted_iota(jnp.int32, (RANK, width), 1) < half
    wide_low = lax.broadcasted_iota(jnp.int32, (width, width), 1) < half
    first = [g[:RANK] for g in grams]
    inverse = inverse_factor(jnp.concatenate(first, axis=0), low)
    first_image = jnp.concatenate([product(f, g) for f, g in zip(first, grams)], axis=0)
    images = product(block_diagonal(inverse, low), first_image)
    turned = images.T
    inverse = inverse_factor(images, low)
    spread = jnp.concatenate([jnp.where(wide_low, turned, 0.0), jnp.where(wide_low, 0.0, turned)], axis=0)
    gram_turned = product(jnp.concatenate(grams, axis=1), spread)
    own_images = product(own, turned)
    pivot_row = jnp.concatenate([piv[0:1, :], piv[1:2, :]], axis=1)
    at_pivot = lax.broadcasted_iota(jnp.int32, (width, width), 0) == jnp.broadcast_to(pivot_row, (width, width))
    rows = jnp.concatenate([turned, gram_turned, own_images], axis=0)
    out = product(rows, block_diagonal(inverse, low), transposed=True)
    basis = out[:width]
    sing = jnp.sqrt(jnp.sum(basis * out[width : 2 * width], axis=0, keepdims=True))
    weight = jnp.sum(jnp.where(at_pivot, basis, 0.0), axis=0, keepdims=True) * math.sqrt(width)
    proj = out[2 * width :] * jnp.broadcast_to(weight, (own.shape[0], width))
    return (
        [sing[:, :half], pltpu.roll(sing, half, 1)[:, :half]],
        [proj[:snaps, :half], pltpu.roll(proj[snaps:], half, 1)[:, :half]],
    )


CHUNKS = 16


def sketch_kernel(snap_ref, sketch_ref, out_ref, snap_buf, sketch_buf, sems):
    step = sketch_buf.shape[0] // CHUNKS
    copies = []
    for i in range(CHUNKS):
        rows = pl.ds(i * step, step)
        pair = (
            pltpu.make_async_copy(snap_ref.at[:, rows], snap_buf.at[:, rows], sems.at[0, i]),
            pltpu.make_async_copy(sketch_ref.at[rows, :], sketch_buf.at[rows, :], sems.at[1, i]),
        )
        for copy in pair:
            copy.start()
        copies.append(pair)
    total = None
    for i in range(CHUNKS):
        for copy in copies[i]:
            copy.wait()
        rows = pl.ds(i * step, step)
        part = jnp.dot(snap_buf[:, rows], sketch_buf[rows, :], preferred_element_type=jnp.float32)
        total = part if i == 0 else total + part
    out_ref[...] = total


def sketch_product(snapshots, sketch_matrix):
    dofs, cols = snapshots.shape
    width = sketch_matrix.shape[1]
    return pl.pallas_call(
        sketch_kernel,
        in_specs=[pl.BlockSpec(memory_space=pltpu.HBM)] * 2,
        out_specs=pl.BlockSpec(memory_space=pltpu.VMEM),
        out_shape=jax.ShapeDtypeStruct((cols, width), jnp.float32),
        scratch_shapes=[
            pltpu.VMEM((cols, dofs), snapshots.dtype),
            pltpu.VMEM((dofs, width), sketch_matrix.dtype),
            pltpu.SemaphoreType.DMA((2, CHUNKS)),
        ],
        compiler_params=pltpu.CompilerParams(vmem_limit_bytes=52 * 2**20),
        name="sketch_product",
    )(snapshots.T, sketch_matrix)


def solve_kernel(windows_here, steps, *refs):
    *block_refs, pivot_ref, singular_ref, projection_ref = refs
    core = lax.axis_index("dof") % 2
    rels = [jnp.where(core == 0, even, odd) for even, odd in steps]
    sing, proj = la_core(lax.axis_index("win"), [r[...] for r in block_refs], rels, pivot_ref[...], windows_here)
    for w in range(windows_here):
        singular_ref[w : w + 1, :] = sing[w]
        projection_ref[w] = proj[w]


def solve(blocks, steps, pivots):
    windows_here = pivots.shape[0]
    snaps = blocks[0].shape[0] // windows_here
    singular, projections = pl.pallas_call(
        lambda *refs: solve_kernel(windows_here, steps, *refs),
        in_specs=[pl.BlockSpec(memory_space=pltpu.VMEM)] * (len(blocks) + 1),
        out_specs=[pl.BlockSpec(memory_space=pltpu.VMEM)] * 2,
        out_shape=[
            jax.ShapeDtypeStruct((windows_here, RANK), jnp.float32),
            jax.ShapeDtypeStruct((windows_here, snaps, RANK), jnp.float32),
        ],
        compiler_params=pltpu.CompilerParams(vmem_limit_bytes=8 * 2**20),
        name="solve_windows",
    )(*blocks, pivots)
    return singular, jnp.transpose(projections, (0, 2, 1))


def solution(mesh):
    win_count, dof_count = mesh.shape["win"], mesh.shape["dof"]

    def send(value, target):
        pairs = []
        for w in range(win_count):
            for d in range(dof_count):
                to_w, to_d = target(w, d)
                pairs.append((w * dof_count + d, to_w * dof_count + to_d))
        return lax.ppermute(value, ("win", "dof"), pairs)

    def swap_cores(value):
        return send(value, lambda w, d: (w, d ^ 1))

    def local(snapshots, sketch_matrix, pivots):
        coeffs = sketch_product(snapshots, sketch_matrix)
        coeffs = coeffs + swap_cores(coeffs)
        step = 2
        while step < dof_count:
            coeffs = coeffs + send(coeffs, lambda w, d: (w, d ^ (step + 1)))
            step *= 2
        blocks = [coeffs]
        steps = [(0, 0)]
        for k in range(1, win_count):
            blocks.append(send(coeffs, lambda w, d: (w ^ k, d ^ 1)))
            steps.append((k, k))
        return solve(blocks, steps, pivots)

    return jax.shard_map(
        local,
        mesh=mesh,
        in_specs=(P("dof", "win"), P("dof", None), P("win", None)),
        out_specs=(P("win", None), P("win", None, None)),
        check_vma=False,
    )
```

```python
import math

import jax
import jax.numpy as jnp
from jax import lax
from jax.experimental import pallas as pl
from jax.experimental.pallas import tpu as pltpu
from jax.sharding import PartitionSpec as P


RANK = 64
T = 8
DOWN = 2.0**-10
def split(x):
    high = x.astype(jnp.bfloat16)
    rest = x - high.astype(jnp.float32)
    mid = rest.astype(jnp.bfloat16)
    return high, mid, (rest - mid.astype(jnp.float32)).astype(jnp.bfloat16)


def product(a, b, transposed=False):
    ah, am, al = split(a) if not isinstance(a, tuple) else a
    bh, bm, bl = split(b) if not isinstance(b, tuple) else b
    axis = 1 if transposed else 0
    left = jnp.concatenate([ah, ah, am, ah, am, al], axis=1)
    right = jnp.concatenate([bh, bm, bh, bl, bm, bh], axis=axis)
    return lax.dot_general(left, right, (((1,), (axis,)), ((), ())), preferred_element_type=jnp.float32)


def sb(v, k):
    return jnp.broadcast_to(v[k:k+1, :], v.shape)


def col(v, k, low, half):
    return jnp.take_along_axis(v, jnp.where(low, k, k + half), axis=1, mode="promise_in_bounds")


def eliminate(gram):
    n = len(gram)
    width = gram[0].shape[1]
    half = width // 2
    lane = lax.broadcasted_iota(jnp.int32, gram[0].shape, 1)
    sub = lax.broadcasted_iota(jnp.int32, gram[0].shape, 0)
    low = lane < half
    column = jnp.where(low, lane, lane - half)
    gram = [g * (DOWN * DOWN) for g in gram]
    ahead = None
    for p in range(n):
        cols = {r: [] for r in range(p, n)}
        first = p if ahead is None else p + 1
        for j in range(T):
            for r in range(first, n):
                cols[r].append(col(gram[r], T * p + j, low, half))
        if ahead is not None:
            cols[p] = ahead
        nxt = None
        if p + 1 < n:
            nxt = [col(gram[p + 1], T * (p + 1) + j, low, half) for j in range(T)]
        done = jnp.logical_and(column >= T * p, column < T * (p + 1))
        gram[p] = jnp.where(done, jnp.where(sub == column - T * p, 1.0, 0.0), gram[p])
        for r in range(p + 1, n):
            gram[r] = jnp.where(done, 0.0, gram[r])
        pivots = None
        diag = cols[p]
        for k in range(0, T, 2):
            top = sb(diag[k], k)
            side = sb(diag[k + 1], k)
            low_right = sb(diag[k + 1], k + 1)
            inv0 = 1.0 / top
            inv1 = top * (1.0 / (top * low_right - side * side))
            ratio = side * inv0
            below = low_right - ratio * side
            pivots = top if pivots is None else jnp.where(sub == k, top, pivots)
            pivots = jnp.where(sub == k + 1, below, pivots)
            heads = {}
            for j in range(k + 2, T):
                head = sb(diag[j], k)
                heads[j] = head, sb(diag[j], k + 1) - ratio * head
            row0 = sb(gram[p], k)
            row1 = sb(gram[p], k + 1) - ratio * row0
            for r in range(p, n):
                m0 = cols[r][k] * inv0
                second = cols[r][k + 1] - m0 * side
                m1 = second * inv1
                for j in range(k + 2, T):
                    cols[r][j] = (cols[r][j] - m0 * heads[j][0]) - m1 * heads[j][1]
                if r == p + 1:
                    for j in range(T):
                        nxt[j] = (nxt[j] - m0 * sb(cols[r][k], j)) - m1 * sb(second, j)
                if r == p:
                    m0 = jnp.where(sub > k, m0, 0.0)
                    m1 = jnp.where(sub > k + 1, m1, 0.0)
                gram[r] = (gram[r] - m0 * row0) - m1 * row1
        gram[p] = jnp.where(column < T * (p + 1), gram[p] * (lax.rsqrt(pivots) * DOWN), 0.0)
        ahead = nxt
    return gram


def tiles(a): return [a[T*i:T*(i+1)] for i in range(a.shape[0]//T)]
def diagonal_blocks(square, low):
    n = square.shape[0] // 2
    return jnp.where(low, square[:n], square[n:])


def block_diagonal(pair, low):
    return jnp.concatenate([jnp.where(low, pair, 0.0), jnp.where(low, 0.0, pair)], axis=0)


def inverse_factor(images, low):
    pair = diagonal_blocks(product(images, images, transposed=True), low)
    return jnp.concatenate(eliminate(tiles(pair)), axis=0)


def la_core(win, blocks, rels, piv, nwin_here):
    width = blocks[0].shape[1]
    half = width // 2
    own = blocks[0]
    snaps = own.shape[0] // 2
    others = [jnp.where(jnp.bitwise_xor(win, rel) < win, b, 0.0) for b, rel in zip(blocks[1:], rels[1:])]
    full = jnp.concatenate(blocks, axis=0)
    kept = [
        jnp.concatenate([own[:snaps], jnp.zeros((snaps, width), jnp.float32)] + others, axis=0),
        jnp.concatenate([own] + others, axis=0),
    ]
    sums = product(full.T, jnp.concatenate(kept, axis=1))
    eye = (
        lax.broadcasted_iota(jnp.int32, (width, width), 0) == lax.broadcasted_iota(jnp.int32, (width, width), 1)
    ).astype(jnp.float32)
    grams = [
        eye + sums[:, width * w : width * (w + 1)] / (snaps * (win * 2 + w + 1)).astype(jnp.float32) for w in range(2)
    ]
    low = lax.broadcasted_iota(jnp.int32, (RANK, width), 1) < half
    wide_low = lax.broadcasted_iota(jnp.int32, (width, width), 1) < half
    first = [g[:RANK] for g in grams]
    inverse = inverse_factor(jnp.concatenate(first, axis=0), low)
    first_image = jnp.concatenate([product(f, g) for f, g in zip(first, grams)], axis=0)
    images = product(block_diagonal(inverse, low), first_image)
    turned = images.T
    inverse = inverse_factor(images, low)
    spread = jnp.concatenate([jnp.where(wide_low, turned, 0.0), jnp.where(wide_low, 0.0, turned)], axis=0)
    gram_turned = product(jnp.concatenate(grams, axis=1), spread)
    own_images = product(own, turned)
    pivot_row = jnp.concatenate([piv[0:1, :], piv[1:2, :]], axis=1)
    at_pivot = lax.broadcasted_iota(jnp.int32, (width, width), 0) == jnp.broadcast_to(pivot_row, (width, width))
    rows = jnp.concatenate([turned, gram_turned, own_images], axis=0)
    out = product(rows, block_diagonal(inverse, low), transposed=True)
    basis = out[:width]
    sing = jnp.sqrt(jnp.sum(basis * out[width : 2 * width], axis=0, keepdims=True))
    weight = jnp.sum(jnp.where(at_pivot, basis, 0.0), axis=0, keepdims=True) * math.sqrt(width)
    proj = out[2 * width :] * jnp.broadcast_to(weight, (own.shape[0], width))
    return (
        [sing[:, :half], pltpu.roll(sing, half, 1)[:, :half]],
        [proj[:snaps, :half], pltpu.roll(proj[snaps:], half, 1)[:, :half]],
    )


CHUNKS = 16


def sketch_kernel(snap_ref, sketch_ref, out_ref, snap_buf, sketch_buf, sems):
    step = sketch_buf.shape[0] // CHUNKS
    copies = []
    for i in range(CHUNKS):
        rows = pl.ds(i * step, step)
        pair = (
            pltpu.make_async_copy(snap_ref.at[:, rows], snap_buf.at[:, rows], sems.at[0, i]),
            pltpu.make_async_copy(sketch_ref.at[rows, :], sketch_buf.at[rows, :], sems.at[1, i]),
        )
        for copy in pair:
            copy.start()
        copies.append(pair)
    total = None
    for i in range(CHUNKS):
        for copy in copies[i]:
            copy.wait()
        rows = pl.ds(i * step, step)
        part = jnp.dot(snap_buf[:, rows], sketch_buf[rows, :], preferred_element_type=jnp.float32)
        total = part if i == 0 else total + part
    out_ref[...] = total


def sketch_product(snapshots, sketch_matrix):
    dofs, cols = snapshots.shape
    width = sketch_matrix.shape[1]
    return pl.pallas_call(
        sketch_kernel,
        in_specs=[pl.BlockSpec(memory_space=pltpu.HBM)] * 2,
        out_specs=pl.BlockSpec(memory_space=pltpu.VMEM),
        out_shape=jax.ShapeDtypeStruct((cols, width), jnp.float32),
        scratch_shapes=[
            pltpu.VMEM((cols, dofs), snapshots.dtype),
            pltpu.VMEM((dofs, width), sketch_matrix.dtype),
            pltpu.SemaphoreType.DMA((2, CHUNKS)),
        ],
        compiler_params=pltpu.CompilerParams(vmem_limit_bytes=52 * 2**20),
        name="sketch_product",
    )(snapshots.T, sketch_matrix)


def solve_kernel(windows_here, steps, *refs):
    *block_refs, pivot_ref, singular_ref, projection_ref = refs
    core = lax.axis_index("dof") % 2
    rels = [jnp.where(core == 0, even, odd) for even, odd in steps]
    sing, proj = la_core(lax.axis_index("win"), [r[...] for r in block_refs], rels, pivot_ref[...], windows_here)
    for w in range(windows_here):
        singular_ref[w : w + 1, :] = sing[w]
        projection_ref[w] = proj[w]


def solve(blocks, steps, pivots):
    windows_here = pivots.shape[0]
    snaps = blocks[0].shape[0] // windows_here
    singular, projections = pl.pallas_call(
        lambda *refs: solve_kernel(windows_here, steps, *refs),
        in_specs=[pl.BlockSpec(memory_space=pltpu.VMEM)] * (len(blocks) + 1),
        out_specs=[pl.BlockSpec(memory_space=pltpu.VMEM)] * 2,
        out_shape=[
            jax.ShapeDtypeStruct((windows_here, RANK), jnp.float32),
            jax.ShapeDtypeStruct((windows_here, snaps, RANK), jnp.float32),
        ],
        compiler_params=pltpu.CompilerParams(vmem_limit_bytes=8 * 2**20),
        name="solve_windows",
    )(*blocks, pivots)
    return singular, jnp.transpose(projections, (0, 2, 1))


def solution(mesh):
    win_count, dof_count = mesh.shape["win"], mesh.shape["dof"]

    def send(value, target):
        pairs = []
        for w in range(win_count):
            for d in range(dof_count):
                to_w, to_d = target(w, d)
                pairs.append((w * dof_count + d, to_w * dof_count + to_d))
        return lax.ppermute(value, ("win", "dof"), pairs)

    def swap_cores(value):
        return send(value, lambda w, d: (w, d ^ 1))

    def local(snapshots, sketch_matrix, pivots):
        coeffs = sketch_product(snapshots, sketch_matrix)
        coeffs = coeffs + swap_cores(coeffs)
        step = 2
        while step < dof_count:
            coeffs = coeffs + send(coeffs, lambda w, d: (w, d ^ (step + 1)))
            step *= 2
        blocks = [coeffs]
        steps = [(0, 0)]
        for k in range(1, win_count):
            blocks.append(send(coeffs, lambda w, d: (w ^ k, d ^ 1)))
            steps.append((k, k))
        return solve(blocks, steps, pivots)

    return jax.shard_map(
        local,
        mesh=mesh,
        in_specs=(P("dof", "win"), P("dof", None), P("win", None)),
        out_specs=(P("win", None), P("win", None, None)),
        check_vma=False,
    )
```
